32 devices in a mesh: gx: 4 (over y, x), gy: 2 (over core), gz: 4 (over z).
Axes of the slice: x: 2, y: 2, z: 4, core: 2. Of those that a mesh axis runs over, the one named last changes fastest.
Arguments:
- residual_in: float32 [256, 128, 1024], P('gx', 'gy', 'gz'), may hold values from -700 to 700
Outputs:
- level_one: float32 [128, 64, 512], P('gx', 'gy', 'gz')
- level_two: float32 [64, 32, 256], P('gx', 'gy', 'gz')
- level_three: float32 [32, 16, 128], P('gx', 'gy', 'gz')
- level_four: float32 [16, 8, 64], P('gx', 'gy', 'gz')
- level_five: float32 [8, 4, 32], P('gx', 'gy', 'gz')
- level_scales: float32 [5], replicated
The draws below stay inside these ranges and needn't reach their ends.
All inputs are finite; a program needn't handle non-finite values.
Results may differ from the reference program's by a relative error of at most 0.0002.
Values sent between devices are 32-bit elements; how exact they have to be, the bound alone decides.
A program may use at most 64 MiB of HBM per device.

```python
import math
import jax
import jax.numpy as jnp
from jax import lax

LEVELS = 5
NX = 256
NY = 128
NZ = 1024


def draw_residual_in(key, part):
    key_list = jax.random.split(key, 5)
    ramp_x = jnp.exp(0.5 * math.log(3.0) * jnp.arange(NX, dtype=jnp.float32) / max(NX - 1, 1))
    ramp_y = jnp.exp(0.5 * math.log(3.0) * jnp.arange(NY, dtype=jnp.float32) / max(NY - 1, 1))
    ramp_z = jnp.exp(0.5 * math.log(3.0) * jnp.arange(NZ, dtype=jnp.float32) / max(NZ - 1, 1))
    rough_x = jnp.exp(0.5 * math.log(10.0) * jax.random.uniform(key_list[0], (NX,), jnp.float32))
    rough_y = jnp.exp(0.5 * math.log(10.0) * jax.random.uniform(key_list[1], (NY,), jnp.float32))
    rough_z = jnp.exp(0.5 * math.log(10.0) * jax.random.uniform(key_list[2], (NZ,), jnp.float32))
    amplitude = (ramp_x * rough_x)[:, None, None] * (ramp_y * rough_y)[None, :, None] * (ramp_z * rough_z)[None, None, :]
    values = amplitude * jax.random.truncated_normal(key_list[4], -4.0, 4.0, (NX, NY, NZ), jnp.float32)
    return values.astype(jnp.float32)


def setup_inputs(seed: int = 0) -> dict:
    arg_keys = jax.random.split(jax.random.key(seed), 2)
    residual_in = draw_residual_in(jax.random.fold_in(arg_keys[1], 71), 0)
    return {"residual_in": residual_in}


WEIGHTS = (0.25, 0.5, 0.25)
EPSILON = 1e-06

def restrict_cube(values):
    half_x = values.shape[0] // 2
    half_y = values.shape[1] // 2
    half_z = values.shape[2] // 2
    padded = jnp.pad(values, ((1, 0), (1, 0), (1, 0)))
    summed = jnp.zeros((half_x, half_y, half_z), jnp.float32)
    for off_x in range(3):
        for off_y in range(3):
            for off_z in range(3):
                picked = lax.slice(padded, (off_x, off_y, off_z), (off_x + 2 * half_x - 1, off_y + 2 * half_y - 1, off_z + 2 * half_z - 1), (2, 2, 2))
                summed = summed + WEIGHTS[off_x] * WEIGHTS[off_y] * WEIGHTS[off_z] * picked
    return summed

def reference(residual_in):
    current = residual_in
    grid_list = []
    scale_list = []
    for step_no in range(LEVELS):
        coarse = restrict_cube(current)
        mean_sq = jnp.sum(coarse * coarse) / coarse.size
        scale_now = jnp.sqrt(mean_sq + EPSILON)
        current = coarse / scale_now
        grid_list.append(current)
        scale_list.append(scale_now)
    return (grid_list[0], grid_list[1], grid_list[2], grid_list[3], grid_list[4], jnp.stack(scale_list))
```

```python
import functools

import jax
import jax.numpy as jnp
import ml_dtypes
import numpy as np
from jax import lax
from jax.experimental import pallas as pl
from jax.experimental.pallas import tpu as pltpu
from jax.sharding import PartitionSpec as P

LEVELS = 5
EPSILON = 1e-06
LANES = 128
PAD = 8
CHUNKS = 4
AXES = ("gx", "gy", "gz")
MESH = pl.DeviceIdType.MESH
HOPS = ((1, 1, 1), (1, 0, 1), (0, 1, 1), (0, 0, 1), (1, 0, 0), (1, 1, 0), (0, 1, 0))


def round_up(n, m):
    return -(-n // m) * m


def step_matrix(n_in, n_cells):
    out = np.zeros((n_cells // 2 + 1, n_in))
    for i in range(n_cells // 2 + 1):
        for off, w in ((-1, 0.25), (0, 0.5), (1, 0.25)):
            if 0 <= 2 * i + off < n_in:
                out[i, 2 * i + off] = w
    return out


def exact(table):
    out = table.astype(np.float32).astype(ml_dtypes.bfloat16)
    assert (out.astype(np.float64) == table).all()
    return out


class Plan:
    def __init__(self, shape):
        self.nx, self.ny, self.nz = shape
        self.xs = [self.nx >> l for l in range(1, LEVELS + 1)]
        self.ys = [self.ny >> l for l in range(1, LEVELS + 1)]
        self.zs = [self.nz >> l for l in range(1, LEVELS + 1)]
        assert self.zs[0] == LANES and self.ys[0] % 8 == 0
        self.ext = [round_up(y + 1, 8) for y in self.ys]
        self.pys = [round_up(y, 8) for y in self.ys]
        self.coff = [0] + np.concatenate([[0], np.cumsum(self.zs[1:])]).tolist()
        self.end = self.coff[-1]
        self.tail = [self.end + LEVELS - 1] + [self.end + l for l in range(LEVELS - 1)]
        assert self.end + LEVELS <= LANES
        self.zoff = np.concatenate([[0], np.cumsum(self.xs)]).tolist()
        assert self.zoff[-1] <= LANES
        rows = [x * p for x, p in zip(self.xs[1:], self.pys[1:])]
        self.base = [0] + np.concatenate([[0], np.cumsum(rows)]).tolist()
        self.own = self.base[-1]
        self.stage = [PAD + max(self.ext[l - 1], 2 * self.ext[l]) for l in range(1, LEVELS)]

    def table(self):
        m = step_matrix(self.nz, self.nz)
        out = np.zeros((self.nz, 2 * LANES))
        out[:, :LANES] = m[:-1].T
        out[:, LANES + self.tail[0]] = m[-1]
        for l in range(1, LEVELS):
            m = step_matrix(self.zs[l - 1] + 1, self.zs[l - 1]) @ m
            at = LANES + self.coff[l]
            out[:, at : at + self.zs[l]] = m[:-1].T
            out[:, LANES + self.tail[l]] = m[-1]
        return exact(out / 16)


def halves(x):
    hi = x.astype(jnp.bfloat16)
    return hi, (x - hi.astype(jnp.float32)).astype(jnp.bfloat16)


def dot(a, b):
    return lax.dot_general(a, b, (((1,), (0,)), ((), ())), preferred_element_type=jnp.float32)


def roll(x, shift):
    shift %= LANES
    return pltpu.roll(x, shift, 1) if shift else x


def gather_kernel(plan, sizes, *refs):
    p = plan
    v_hbm, table_hbm = refs[:2]
    out1_hbm, outc_hbm, stats = refs[2:5]
    vin, table = refs[5:7]
    stages = refs[7:11]
    sends = refs[11:18]
    recvs = refs[18:25]
    mine, parts = refs[25:27]
    vsem, tsem, ssem, rsem, asend, arecv = refs[27:33]
    out1, outc, osem = refs[33:36]
    f32 = jnp.float32
    pos = [lax.axis_index(a) for a in AXES]
    group = sizes[0] * sizes[1]
    me = pos[0] * sizes[1] + pos[1]
    x1, y1 = p.xs[0], p.ys[0]

    in_plane = []
    for k in range(group):
        r = lax.rem(me + k, group)
        in_plane.append((r // sizes[1], lax.rem(r, sizes[1])))
    in_line = [lax.rem(pos[2] + k, sizes[2]) for k in range(sizes[2])]
    others = [
        {"gx": gx, "gy": gy, "gz": gz} for gz in in_line for gx, gy in in_plane
    ][1:]

    def along(hop, way):
        ok, target = None, {}
        for a in range(3):
            target[AXES[a]] = pos[a]
            if hop[a]:
                here = pos[a] < sizes[a] - 1 if way > 0 else pos[a] > 0
                ok = here if ok is None else jnp.logical_and(ok, here)
                target[AXES[a]] = lax.rem(pos[a] + way + sizes[a], sizes[a])
        return ok, target

    per = p.nx // CHUNKS
    tcopy = pltpu.make_async_copy(table_hbm, table, tsem.at[0])
    vcopies = [
        [
            pltpu.make_async_copy(
                v_hbm.at[pl.ds(c * per, per), :, pl.ds(h * LANES, LANES)],
                vin.at[pl.ds(c * per, per), h, pl.ds(PAD, p.ny)],
                vsem.at[2 * c + h],
            )
            for h in range(2)
        ]
        for c in range(CHUNKS)
    ]
    for pair in vcopies[:1]:
        for c in pair:
            c.start()
    tcopy.start()
    for pair in vcopies[1:]:
        for c in pair:
            c.start()

    barrier = pltpu.get_barrier_semaphore()
    for target in others:
        pl.semaphore_signal(barrier, inc=1, device_id=target, device_id_type=MESH)

    after = PAD + p.ny
    for x in range(p.nx):
        for h in range(2):
            vin[x, h, 0:PAD, :] = jnp.zeros((PAD, LANES), f32)
            vin[x, h, after:, :] = jnp.zeros((2 * PAD, LANES), f32)
    for l in range(1, LEVELS):
        s = stages[l - 1]
        for k in range(p.xs[l] + 1):
            s[k, 0:PAD, :] = jnp.zeros((PAD, LANES), f32)
            rest = p.stage[l - 1] - PAD - p.ext[l - 1]
            if rest:
                s[k, PAD + p.ext[l - 1] :, :] = jnp.zeros((rest, LANES), f32)

    def plane_of(x):
        cols = []
        for h in range(2):
            even = vin[x, h, pl.ds(PAD, y1, 2), :]
            odd = vin[x, h, pl.ds(PAD + 1, y1, 2), :]
            prev = vin[x, h, pl.ds(PAD - 1, y1, 2), :]
            last = vin[x, h, pl.ds(after - 1, 8, 2), :]
            cols.append(jnp.concatenate([(even + even) + (odd + prev), last], axis=0))
        return jnp.concatenate(cols, axis=1)

    def lanes_of(n):
        return lax.broadcasted_iota(jnp.int32, (n, LANES), 1)

    def fold_x(planes, k, n):
        if k == n:
            return 0.25 * planes[2 * k - 1] + 0.5 * planes[2 * k]
        sides = planes[2 * k + 1] + planes[2 * k - 1] if k else planes[1]
        return 0.5 * planes[2 * k] + 0.25 * sides

    def fold_y(s, k, n):
        even = s[k, pl.ds(PAD, n, 2), :]
        odd = s[k, pl.ds(PAD + 1, n, 2), :]
        prev = s[k, pl.ds(PAD - 1, n, 2), :]
        return 0.5 * even + 0.25 * (odd + prev)

    xyz, zx, yz, zf, xf, xy, yf = sends
    half = per // 2
    rows = p.ext[0]
    lane = lanes_of(rows)
    comps = []
    columns = [jnp.zeros((e, LANES), f32) for e in p.ext]
    before = None
    tcopy.wait()
    for c in range(CHUNKS):
        for copy in vcopies[c]:
            copy.wait()
        us = []
        for j in range(half):
            i = c * half + j
            even, odd = plane_of(2 * i), plane_of(2 * i + 1)
            t = (even + even) + odd
            us.append(t if before is None else t + before)
            before = odd
        if c == CHUNKS - 1:
            us.append(before)
        count = len(us)
        if count * rows % 16:
            us.append(jnp.zeros((8, p.nz), f32))
        hi, lo = halves(jnp.concatenate(us, axis=0))
        z = dot(hi, table[...]) + dot(lo, table[...])
        for j in range(count):
            i = c * half + j
            plane = z[j * rows : (j + 1) * rows]
            comp = plane[:, LANES:]
            comps.append(comp)
            moved = roll(comp, (i % x1) - p.tail[0])
            if i < x1:
                out1[i] = plane[:y1, :LANES]
                yf[i : i + 1, :] = plane[y1 : y1 + 1, :LANES]
                columns[0] = jnp.where(lane == i, moved, columns[0])
            else:
                xf[0:y1, :] = plane[:y1, :LANES]
                xy[0:1, :] = plane[y1 : y1 + 1, :LANES]
                corners = [jnp.where(lane == 0, moved, 0.0)]
            if i % 2 or i == x1:
                stages[0][i // 2, PAD : PAD + rows, :] = fold_x(comps, i // 2, p.xs[1])

    grids = [None]
    for l in range(1, LEVELS):
        n, e = p.xs[l], p.ext[l]
        planes = [fold_y(stages[l - 1], k, e) for k in range(n + 1)]
        lane = lanes_of(e)
        for k in range(n + 1):
            to = p.zoff[l] + k % n
            moved = roll(planes[k], to - p.tail[l])
            if k < n:
                columns[l] = jnp.where(lane == to, moved, columns[l])
            else:
                corners.append(jnp.where(lane == to, moved, 0.0))
        grids.append(planes)
        if l + 1 < LEVELS:
            for k in range(p.xs[l + 1] + 1):
                stages[l][k, PAD : PAD + e, :] = fold_x(planes, k, p.xs[l + 1])

    def pick(pieces):
        n = pieces[0][1].shape[0]
        lane = lanes_of(n)
        out = pieces[0][1]
        for l, x in pieces[1:]:
            out = jnp.where(lane >= p.coff[l], x, out)
        return out

    def face(cols, dst, edge):
        for g in range(y1 // 8):
            dst[8 * g : 8 * g + 8, :] = functools.reduce(
                jnp.add, [t[8 * g : 8 * g + 8] for t in cols if 8 * g + 8 <= t.shape[0]]
            )
        line = functools.reduce(
            jnp.add, [t[y : y + 1] for t, y in zip(cols, p.ys)]
        )
        top = lax.broadcasted_iota(jnp.int32, (8, LANES), 0) == 0
        edge[...] = jnp.where(top, line, 0.0)

    face(corners, zx, xyz)
    face(columns, zf, yz)
    levels = range(1, LEVELS)
    for g in range(p.pys[1] // 8):
        at = y1 + 8 * g
        xf[at : at + 8, :] = pick(
            [
                (l, grids[l][p.xs[l]][8 * g : 8 * g + 8])
                for l in levels
                if 8 * g + 8 <= p.pys[l]
            ]
        )
    xy[1:2, :] = pick([(l, grids[l][p.xs[l]][p.ys[l] : p.ys[l] + 1]) for l in levels])
    for k in range(p.xs[1]):
        yf[x1 + k : x1 + k + 1, :] = pick(
            [(l, grids[l][k][p.ys[l] : p.ys[l] + 1]) for l in levels if k < p.xs[l]]
        )
    for l in levels:
        q = p.pys[l]
        for k in range(p.xs[l]):
            outc[p.base[l] + k * q : p.base[l] + (k + 1) * q, :] = grids[l][k][:q]

    pl.semaphore_wait(barrier, len(others))

    has_next, has_prev, copies = [], [], []
    for n, hop in enumerate(HOPS):
        ok_n, target = along(hop, 1)
        has_next.append(ok_n)
        has_prev.append(along(hop, -1)[0])
        copies.append(
            pltpu.make_async_remote_copy(
                src_ref=sends[n],
                dst_ref=recvs[n],
                send_sem=ssem.at[n],
                recv_sem=rsem.at[n],
                device_id=target,
                device_id_type=MESH,
            )
        )
    for n in range(len(HOPS)):

        @pl.when(has_next[n])
        def _():
            copies[n].start()

    for n in range(len(HOPS)):

        @pl.when(jnp.logical_not(has_prev[n]))
        def _():
            recvs[n][...] = jnp.zeros(recvs[n].shape, f32)

    for n in range(len(HOPS)):

        @pl.when(has_prev[n])
        def _():
            copies[n].wait_recv()

    rxyz, rzx, ryz, rzf, rxf, rxy, ryf = recvs
    col = [rzf[8 * g : 8 * g + 8, :] + rzx[8 * g : 8 * g + 8, :] for g in range(y1 // 8)]
    col[0] = col[0] + ryz[...] + rxyz[...]
    top = lax.broadcasted_iota(jnp.int32, (8, LANES), 0) == 0
    row = lax.broadcasted_iota(jnp.int32, (8, LANES), 0)
    lane = lanes_of(8)
    acc = jnp.zeros((8, LANES), f32)
    for i in range(x1):
        edge = ryf[i : i + 1, :]
        if i == 0:
            edge = edge + rxy[0:1, :]
        for g in range(y1 // 8):
            part = out1[i, 8 * g : 8 * g + 8, :]
            if i == 0:
                part = part + rxf[8 * g : 8 * g + 8, :]
            if g == 0:
                part = part + jnp.where(top, edge, 0.0)
            part = part + jnp.where(lane == 0, roll(col[g], -i), 0.0)
            out1[i, 8 * g : 8 * g + 8, :] = part
            acc = acc + part * part
    results = [
        pltpu.make_async_copy(out1, out1_hbm, osem.at[0]),
        pltpu.make_async_copy(outc, outc_hbm, osem.at[1]),
    ]
    results[0].start()
    mine[0:1, :] = jnp.sum(acc, axis=0, keepdims=True)
    acc = jnp.zeros((8, LANES), f32)
    for l in levels:
        q = p.pys[l]
        keep = (lane >= p.coff[l]) & (lane < p.coff[l + 1] if l + 1 < LEVELS else lane < p.end)
        if p.ys[l] < 8:
            keep = keep & (row < p.ys[l])
        total = jnp.zeros((8, LANES), f32)
        for k in range(p.xs[l]):
            edge = ryf[x1 + k : x1 + k + 1, :]
            if k == 0:
                edge = edge + rxy[1:2, :]
            for g in range(q // 8):
                at = p.base[l] + k * q + 8 * g
                part = outc[at : at + 8, :]
                if k == 0:
                    part = part + rxf[y1 + 8 * g : y1 + 8 * g + 8, :]
                if g == 0:
                    part = part + jnp.where(top, edge, 0.0)
                shifted = roll(col[g], p.coff[l] - p.zoff[l] - k)
                part = part + jnp.where(lane == p.coff[l], shifted, 0.0)
                outc[at : at + 8, :] = part
                total = total + part * part
        acc = jnp.where(keep, total, acc)
    mine[1:2, :] = jnp.sum(acc, axis=0, keepdims=True)
    results[1].start()

    pending = [
        pltpu.make_async_remote_copy(
            src_ref=mine,
            dst_ref=parts.at[k + 1],
            send_sem=asend.at[k],
            recv_sem=arecv.at[k],
            device_id=target,
            device_id_type=MESH,
        )
        for k, target in enumerate(others)
    ]
    for c in reversed(pending):
        c.start()
    parts[0] = mine[...]
    for c in pending:
        c.wait_recv()
    stats[...] = jnp.sum(parts[...], axis=0)
    for c in results:
        c.wait()
    for c in pending:
        c.wait_send()
    for n in range(len(HOPS)):

        @pl.when(has_next[n])
        def _():
            copies[n].wait_send()


def scale_kernel(plan, devices, grid, packed, stats, o1, o2, o3, o4, o5, scales):
    p = plan
    lane1 = lax.broadcasted_iota(jnp.int32, (1, LANES), 1)
    outs = (o1, o2, o3, o4, o5)
    product = jnp.ones((1, 1), jnp.float32)
    for l in range(LEVELS):
        row = stats[0:1, :] if l == 0 else stats[1:2, :]
        if l:
            end = p.coff[l] + p.zs[l]
            row = jnp.where((lane1 >= p.coff[l]) & (lane1 < end), row, 0.0)
        total = jnp.sum(row, axis=1, keepdims=True)
        cells = devices * p.xs[l] * p.ys[l] * p.zs[l]
        scale = jnp.sqrt(total / (product * product) / cells + EPSILON)
        product = product * scale
        scales[l] = scale[0, 0]
        inverse = 1.0 / product
        if l == 0:
            o1[...] = grid[...] * inverse.reshape(1, 1, 1)
            continue
        block = packed[p.base[l] : p.base[l + 1], :] * inverse
        block = roll(block, -p.coff[l])
        block = block.reshape(p.xs[l], p.pys[l], LANES)
        outs[l][...] = block[:, : p.ys[l], : p.zs[l]]


def per_device(sizes, residual_in):
    plan = Plan(residual_in.shape)
    p = plan
    count = sizes[0] * sizes[1] * sizes[2]
    f32, bf16 = jnp.float32, jnp.bfloat16
    long = p.ys[0] + p.pys[1]
    messages = [(8, LANES), (p.ys[0], LANES), (8, LANES), (p.ys[0], LANES)]
    messages += [(long, LANES), (8, LANES), (p.xs[0] + p.xs[1], LANES)]
    anywhere = pl.BlockSpec(memory_space=pl.ANY)
    vmem = pl.BlockSpec(memory_space=pltpu.VMEM)
    dma = pltpu.SemaphoreType.DMA
    grid, packed, stats = pl.pallas_call(
        functools.partial(gather_kernel, p, sizes),
        out_shape=(
            jax.ShapeDtypeStruct((p.xs[0], p.ys[0], p.zs[0]), f32),
            jax.ShapeDtypeStruct((p.own, LANES), f32),
            jax.ShapeDtypeStruct((2, LANES), f32),
        ),
        in_specs=[anywhere] * 2,
        out_specs=(anywhere, anywhere, vmem),
        scratch_shapes=[
            pltpu.VMEM((p.nx, 2, p.ny + 3 * PAD, LANES), f32),
            pltpu.VMEM((p.nz, 2 * LANES), bf16),
        ]
        + [pltpu.VMEM((p.xs[l] + 1, p.stage[l - 1], LANES), f32) for l in range(1, LEVELS)]
        + [pltpu.VMEM(s, f32) for s in messages]
        + [pltpu.VMEM(s, f32) for s in messages]
        + [
            pltpu.VMEM((2, LANES), f32),
            pltpu.VMEM((count, 2, LANES), f32),
            dma((2 * CHUNKS,)),
            dma((1,)),
            dma((len(HOPS),)),
            dma((len(HOPS),)),
            dma((count - 1,)),
            dma((count - 1,)),
            pltpu.VMEM((p.xs[0], p.ys[0], p.zs[0]), f32),
            pltpu.VMEM((p.own, LANES), f32),
            dma((2,)),
        ],
        compiler_params=pltpu.CompilerParams(collective_id=0, has_side_effects=True),
        name="restrict_exchange",
    )(residual_in, jnp.asarray(p.table()))
    shapes = list(zip(p.xs, p.ys, p.zs))
    return pl.pallas_call(
        functools.partial(scale_kernel, p, count),
        out_shape=tuple(jax.ShapeDtypeStruct(s, f32) for s in shapes)
        + (jax.ShapeDtypeStruct((LEVELS,), f32),),
        in_specs=[vmem] * 3,
        out_specs=(vmem,) * 5 + (pl.BlockSpec(memory_space=pltpu.SMEM),),
        name="scale_levels",
    )(grid, packed, stats)


def solution(mesh):
    sizes = tuple(mesh.shape[a] for a in AXES)
    spec = P(*AXES)
    return jax.shard_map(
        functools.partial(per_device, sizes),
        mesh=mesh,
        in_specs=(spec,),
        out_specs=(spec,) * 5 + (P(),),
        check_vma=False,
    )
```

```python
import functools

import jax
import jax.numpy as jnp
import numpy as np
from jax import lax
from jax.experimental import pallas as pl
from jax.experimental.pallas import tpu as pltpu
from jax.sharding import PartitionSpec as P

LEVELS = 5
EPSILON = 1e-06
LANES = 128
PAD = 8
CHUNKS = 4
AXES = ("gx", "gy", "gz")
MESH = pl.DeviceIdType.MESH
HOPS = ((1, 1, 1), (1, 0, 1), (0, 1, 1), (0, 0, 1), (1, 0, 0), (1, 1, 0), (0, 1, 0))


def round_up(n, m):
    return -(-n // m) * m


class Plan:
    def __init__(self, shape):
        self.nx, self.ny, self.nz = shape
        self.xs = [self.nx >> l for l in range(1, LEVELS + 1)]
        self.ys = [self.ny >> l for l in range(1, LEVELS + 1)]
        self.zs = [self.nz >> l for l in range(1, LEVELS + 1)]
        assert self.zs[0] == LANES and self.ys[0] % 8 == 0
        self.ext = [round_up(y + 1, 8) for y in self.ys]
        self.pys = [round_up(y, 8) for y in self.ys]
        self.coff = [0] + np.concatenate([[0], np.cumsum(self.zs[1:])]).tolist()
        self.end = self.coff[-1]
        self.tail = [self.end + LEVELS - 1] + [self.end + l for l in range(LEVELS - 1)]
        assert self.end + LEVELS <= LANES
        self.zoff = np.concatenate([[0], np.cumsum(self.xs)]).tolist()
        assert self.zoff[-1] <= LANES
        rows = [x * p for x, p in zip(self.xs[1:], self.pys[1:])]
        self.base = [0] + np.concatenate([[0], np.cumsum(rows)]).tolist()
        self.own = self.base[-1]
        self.stage = [PAD + max(self.ext[l - 1], 2 * self.ext[l]) for l in range(1, LEVELS)]

    def fill(self, table):
        col = lax.broadcasted_iota(jnp.int32, (1, 2 * LANES), 1)
        width = jnp.full((1, 2 * LANES), 2, jnp.int32)
        cell = col
        for l in range(1, LEVELS):
            inside = col >= LANES + self.coff[l]
            width = jnp.where(inside, 2 << l, width)
            cell = jnp.where(inside, col - (LANES + self.coff[l]), cell)
        for l in range(LEVELS):
            inside = col == LANES + self.tail[l]
            width = jnp.where(inside, 2 << l, width)
            cell = jnp.where(inside, self.zs[l], cell)
        inside = (col < LANES + self.end + LEVELS).astype(jnp.float32)
        at, width = (width * cell).astype(jnp.float32), width.astype(jnp.float32)
        factor = inside / (16.0 * width * width)
        step = 64
        for r in range(0, self.nz, step):
            z = lax.broadcasted_iota(jnp.int32, (step, 2 * LANES), 0) + r
            hat = jnp.maximum(width - jnp.abs(z.astype(jnp.float32) - at), 0.0)
            table[r : r + step, :] = (hat * factor).astype(jnp.bfloat16)


def halves(x):
    hi = x.astype(jnp.bfloat16)
    return hi, (x - hi.astype(jnp.float32)).astype(jnp.bfloat16)


def dot(a, b):
    return lax.dot_general(a, b, (((1,), (0,)), ((), ())), preferred_element_type=jnp.float32)


def roll(x, shift):
    shift %= LANES
    return pltpu.roll(x, shift, 1) if shift else x


def gather_kernel(plan, sizes, *refs):
    p = plan
    v_hbm = refs[0]
    out1, outc, stats = refs[1:4]
    vin, table = refs[4:6]
    stages = refs[6:10]
    sends = refs[10:17]
    recvs = refs[17:24]
    mine, parts = refs[24:26]
    vsem, ssem, rsem, asend, arecv = refs[26:31]
    f32 = jnp.float32
    pos = [lax.axis_index(a) for a in AXES]
    group = sizes[0] * sizes[1]
    me = pos[0] * sizes[1] + pos[1]
    x1, y1 = p.xs[0], p.ys[0]

    in_plane = []
    for k in range(group):
        r = lax.rem(me + k, group)
        in_plane.append((r // sizes[1], lax.rem(r, sizes[1])))
    in_line = [lax.rem(pos[2] + k, sizes[2]) for k in range(sizes[2])]
    others = [
        {"gx": gx, "gy": gy, "gz": gz} for gz in in_line for gx, gy in in_plane
    ][1:]

    def along(hop, way):
        ok, target = None, {}
        for a in range(3):
            target[AXES[a]] = pos[a]
            if hop[a]:
                here = pos[a] < sizes[a] - 1 if way > 0 else pos[a] > 0
                ok = here if ok is None else jnp.logical_and(ok, here)
                target[AXES[a]] = lax.rem(pos[a] + way + sizes[a], sizes[a])
        return ok, target

    per = p.nx // CHUNKS
    vcopies = [
        [
            pltpu.make_async_copy(
                v_hbm.at[pl.ds(c * per, per), :, pl.ds(h * LANES, LANES)],
                vin.at[pl.ds(c * per, per), h, pl.ds(PAD, p.ny)],
                vsem.at[2 * c + h],
            )
            for h in range(2)
        ]
        for c in range(CHUNKS)
    ]
    for pair in vcopies:
        for c in pair:
            c.start()

    barrier = pltpu.get_barrier_semaphore()
    for target in others:
        pl.semaphore_signal(barrier, inc=1, device_id=target, device_id_type=MESH)

    p.fill(table)
    after = PAD + p.ny
    for x in range(p.nx):
        for h in range(2):
            vin[x, h, 0:PAD, :] = jnp.zeros((PAD, LANES), f32)
            vin[x, h, after:, :] = jnp.zeros((2 * PAD, LANES), f32)
    for l in range(1, LEVELS):
        s = stages[l - 1]
        for k in range(p.xs[l] + 1):
            s[k, 0:PAD, :] = jnp.zeros((PAD, LANES), f32)
            rest = p.stage[l - 1] - PAD - p.ext[l - 1]
            if rest:
                s[k, PAD + p.ext[l - 1] :, :] = jnp.zeros((rest, LANES), f32)

    def plane_of(x):
        cols = []
        for h in range(2):
            even = vin[x, h, pl.ds(PAD, y1, 2), :]
            odd = vin[x, h, pl.ds(PAD + 1, y1, 2), :]
            prev = vin[x, h, pl.ds(PAD - 1, y1, 2), :]
            last = vin[x, h, pl.ds(after - 1, 8, 2), :]
            cols.append(jnp.concatenate([(even + even) + (odd + prev), last], axis=0))
        return jnp.concatenate(cols, axis=1)

    def lanes_of(n):
        return lax.broadcasted_iota(jnp.int32, (n, LANES), 1)

    def fold_x(planes, k, n):
        if k == n:
            return 0.25 * planes[2 * k - 1] + 0.5 * planes[2 * k]
        sides = planes[2 * k + 1] + planes[2 * k - 1] if k else planes[1]
        return 0.5 * planes[2 * k] + 0.25 * sides

    def fold_y(s, k, n):
        even = s[k, pl.ds(PAD, n, 2), :]
        odd = s[k, pl.ds(PAD + 1, n, 2), :]
        prev = s[k, pl.ds(PAD - 1, n, 2), :]
        return 0.5 * even + 0.25 * (odd + prev)

    xyz, zx, yz, zf, xf, xy, yf = sends
    half = per // 2
    rows = p.ext[0]
    lane = lanes_of(rows)
    comps = []
    columns = [jnp.zeros((e, LANES), f32) for e in p.ext]
    before = None
    for c in range(CHUNKS):
        for copy in vcopies[c]:
            copy.wait()
        us = []
        for j in range(half):
            i = c * half + j
            even, odd = plane_of(2 * i), plane_of(2 * i + 1)
            t = (even + even) + odd
            us.append(t if before is None else t + before)
            before = odd
        if c == CHUNKS - 1:
            us.append(before)
        count = len(us)
        if count * rows % 16:
            us.append(jnp.zeros((8, p.nz), f32))
        hi, lo = halves(jnp.concatenate(us, axis=0))
        z = dot(hi, table[...]) + dot(lo, table[...])
        for j in range(count):
            i = c * half + j
            plane = z[j * rows : (j + 1) * rows]
            comp = plane[:, LANES:]
            comps.append(comp)
            moved = roll(comp, (i % x1) - p.tail[0])
            if i < x1:
                out1[i] = plane[:y1, :LANES]
                yf[i : i + 1, :] = plane[y1 : y1 + 1, :LANES]
                columns[0] = jnp.where(lane == i, moved, columns[0])
            else:
                xf[0:y1, :] = plane[:y1, :LANES]
                xy[0:1, :] = plane[y1 : y1 + 1, :LANES]
                corners = [jnp.where(lane == 0, moved, 0.0)]
            if i % 2 or i == x1:
                stages[0][i // 2, PAD : PAD + rows, :] = fold_x(comps, i // 2, p.xs[1])

    grids = [None]
    for l in range(1, LEVELS):
        n, e = p.xs[l], p.ext[l]
        planes = [fold_y(stages[l - 1], k, e) for k in range(n + 1)]
        lane = lanes_of(e)
        for k in range(n + 1):
            to = p.zoff[l] + k % n
            moved = roll(planes[k], to - p.tail[l])
            if k < n:
                columns[l] = jnp.where(lane == to, moved, columns[l])
            else:
                corners.append(jnp.where(lane == to, moved, 0.0))
        grids.append(planes)
        if l + 1 < LEVELS:
            for k in range(p.xs[l + 1] + 1):
                stages[l][k, PAD : PAD + e, :] = fold_x(planes, k, p.xs[l + 1])

    def pick(pieces):
        n = pieces[0][1].shape[0]
        lane = lanes_of(n)
        out = pieces[0][1]
        for l, x in pieces[1:]:
            out = jnp.where(lane >= p.coff[l], x, out)
        return out

    def face(cols, dst, edge):
        for g in range(y1 // 8):
            dst[8 * g : 8 * g + 8, :] = functools.reduce(
                jnp.add, [t[8 * g : 8 * g + 8] for t in cols if 8 * g + 8 <= t.shape[0]]
            )
        line = functools.reduce(
            jnp.add, [t[y : y + 1] for t, y in zip(cols, p.ys)]
        )
        top = lax.broadcasted_iota(jnp.int32, (8, LANES), 0) == 0
        edge[...] = jnp.where(top, line, 0.0)

    face(corners, zx, xyz)
    face(columns, zf, yz)
    levels = range(1, LEVELS)
    for g in range(p.pys[1] // 8):
        at = y1 + 8 * g
        xf[at : at + 8, :] = pick(
            [
                (l, grids[l][p.xs[l]][8 * g : 8 * g + 8])
                for l in levels
                if 8 * g + 8 <= p.pys[l]
            ]
        )
    xy[1:2, :] = pick([(l, grids[l][p.xs[l]][p.ys[l] : p.ys[l] + 1]) for l in levels])
    for k in range(p.xs[1]):
        yf[x1 + k : x1 + k + 1, :] = pick(
            [(l, grids[l][k][p.ys[l] : p.ys[l] + 1]) for l in levels if k < p.xs[l]]
        )
    for l in levels:
        q = p.pys[l]
        for k in range(p.xs[l]):
            outc[p.base[l] + k * q : p.base[l] + (k + 1) * q, :] = grids[l][k][:q]

    pl.semaphore_wait(barrier, len(others))

    has_next, has_prev, copies = [], [], []
    for n, hop in enumerate(HOPS):
        ok_n, target = along(hop, 1)
        has_next.append(ok_n)
        has_prev.append(along(hop, -1)[0])
        copies.append(
            pltpu.make_async_remote_copy(
                src_ref=sends[n],
                dst_ref=recvs[n],
                send_sem=ssem.at[n],
                recv_sem=rsem.at[n],
                device_id=target,
                device_id_type=MESH,
            )
        )
    for n in range(len(HOPS)):

        @pl.when(has_next[n])
        def _():
            copies[n].start()

    for n in range(len(HOPS)):

        @pl.when(jnp.logical_not(has_prev[n]))
        def _():
            recvs[n][...] = jnp.zeros(recvs[n].shape, f32)

    for n in range(len(HOPS)):

        @pl.when(has_prev[n])
        def _():
            copies[n].wait_recv()

    rxyz, rzx, ryz, rzf, rxf, rxy, ryf = recvs
    col = [rzf[8 * g : 8 * g + 8, :] + rzx[8 * g : 8 * g + 8, :] for g in range(y1 // 8)]
    col[0] = col[0] + ryz[...] + rxyz[...]
    top = lax.broadcasted_iota(jnp.int32, (8, LANES), 0) == 0
    row = lax.broadcasted_iota(jnp.int32, (8, LANES), 0)
    lane = lanes_of(8)
    acc = jnp.zeros((8, LANES), f32)
    for i in range(x1):
        edge = ryf[i : i + 1, :]
        if i == 0:
            edge = edge + rxy[0:1, :]
        for g in range(y1 // 8):
            part = out1[i, 8 * g : 8 * g + 8, :]
            if i == 0:
                part = part + rxf[8 * g : 8 * g + 8, :]
            if g == 0:
                part = part + jnp.where(top, edge, 0.0)
            part = part + jnp.where(lane == 0, roll(col[g], -i), 0.0)
            out1[i, 8 * g : 8 * g + 8, :] = part
            acc = acc + part * part
    mine[0:1, :] = jnp.sum(acc, axis=0, keepdims=True)
    acc = jnp.zeros((8, LANES), f32)
    for l in levels:
        q = p.pys[l]
        keep = (lane >= p.coff[l]) & (lane < p.coff[l + 1] if l + 1 < LEVELS else lane < p.end)
        if p.ys[l] < 8:
            keep = keep & (row < p.ys[l])
        total = jnp.zeros((8, LANES), f32)
        for k in range(p.xs[l]):
            edge = ryf[x1 + k : x1 + k + 1, :]
            if k == 0:
                edge = edge + rxy[1:2, :]
            for g in range(q // 8):
                at = p.base[l] + k * q + 8 * g
                part = outc[at : at + 8, :]
                if k == 0:
                    part = part + rxf[y1 + 8 * g : y1 + 8 * g + 8, :]
                if g == 0:
                    part = part + jnp.where(top, edge, 0.0)
                shifted = roll(col[g], p.coff[l] - p.zoff[l] - k)
                part = part + jnp.where(lane == p.coff[l], shifted, 0.0)
                outc[at : at + 8, :] = part
                total = total + part * part
        acc = jnp.where(keep, total, acc)
    mine[1:2, :] = jnp.sum(acc, axis=0, keepdims=True)

    pending = [
        pltpu.make_async_remote_copy(
            src_ref=mine,
            dst_ref=parts.at[k + 1],
            send_sem=asend.at[k],
            recv_sem=arecv.at[k],
            device_id=target,
            device_id_type=MESH,
        )
        for k, target in enumerate(others)
    ]
    for c in reversed(pending):
        c.start()
    parts[0] = mine[...]
    for c in pending:
        c.wait_recv()
    stats[...] = jnp.sum(parts[...], axis=0)
    for c in pending:
        c.wait_send()
    for n in range(len(HOPS)):

        @pl.when(has_next[n])
        def _():
            copies[n].wait_send()


def scale_kernel(plan, devices, grid, packed, stats, o1, o2, o3, o4, o5, scales):
    p = plan
    lane1 = lax.broadcasted_iota(jnp.int32, (1, LANES), 1)
    outs = (o1, o2, o3, o4, o5)
    product = jnp.ones((1, 1), jnp.float32)
    for l in range(LEVELS):
        row = stats[0:1, :] if l == 0 else stats[1:2, :]
        if l:
            end = p.coff[l] + p.zs[l]
            row = jnp.where((lane1 >= p.coff[l]) & (lane1 < end), row, 0.0)
        total = jnp.sum(row, axis=1, keepdims=True)
        cells = devices * p.xs[l] * p.ys[l] * p.zs[l]
        scale = jnp.sqrt(total / (product * product) / cells + EPSILON)
        product = product * scale
        scales[l] = scale[0, 0]
        inverse = 1.0 / product
        if l == 0:
            o1[...] = grid[...] * inverse.reshape(1, 1, 1)
            continue
        block = packed[p.base[l] : p.base[l + 1], :] * inverse
        block = roll(block, -p.coff[l])
        block = block.reshape(p.xs[l], p.pys[l], LANES)
        outs[l][...] = block[:, : p.ys[l], : p.zs[l]]


def per_device(sizes, residual_in):
    plan = Plan(residual_in.shape)
    p = plan
    count = sizes[0] * sizes[1] * sizes[2]
    f32, bf16 = jnp.float32, jnp.bfloat16
    long = p.ys[0] + p.pys[1]
    messages = [(8, LANES), (p.ys[0], LANES), (8, LANES), (p.ys[0], LANES)]
    messages += [(long, LANES), (8, LANES), (p.xs[0] + p.xs[1], LANES)]
    anywhere = pl.BlockSpec(memory_space=pl.ANY)
    vmem = pl.BlockSpec(memory_space=pltpu.VMEM)
    dma = pltpu.SemaphoreType.DMA
    grid, packed, stats = pl.pallas_call(
        functools.partial(gather_kernel, p, sizes),
        out_shape=(
            jax.ShapeDtypeStruct((p.xs[0], p.ys[0], p.zs[0]), f32),
            jax.ShapeDtypeStruct((p.own, LANES), f32),
            jax.ShapeDtypeStruct((2, LANES), f32),
        ),
        in_specs=[anywhere],
        out_specs=(vmem, vmem, vmem),
        scratch_shapes=[
            pltpu.VMEM((p.nx, 2, p.ny + 3 * PAD, LANES), f32),
            pltpu.VMEM((p.nz, 2 * LANES), bf16),
        ]
        + [pltpu.VMEM((p.xs[l] + 1, p.stage[l - 1], LANES), f32) for l in range(1, LEVELS)]
        + [pltpu.VMEM(s, f32) for s in messages]
        + [pltpu.VMEM(s, f32) for s in messages]
        + [
            pltpu.VMEM((2, LANES), f32),
            pltpu.VMEM((count, 2, LANES), f32),
            dma((2 * CHUNKS,)),
            dma((len(HOPS),)),
            dma((len(HOPS),)),
            dma((count - 1,)),
            dma((count - 1,)),
        ],
        compiler_params=pltpu.CompilerParams(
            collective_id=0, has_side_effects=True, vmem_limit_bytes=51 << 20
        ),
        name="restrict_exchange",
    )(residual_in)
    shapes = list(zip(p.xs, p.ys, p.zs))
    return pl.pallas_call(
        functools.partial(scale_kernel, p, count),
        out_shape=tuple(jax.ShapeDtypeStruct(s, f32) for s in shapes)
        + (jax.ShapeDtypeStruct((LEVELS,), f32),),
        in_specs=[vmem] * 3,
        out_specs=(vmem,) * 5 + (pl.BlockSpec(memory_space=pltpu.SMEM),),
        compiler_params=pltpu.CompilerParams(vmem_limit_bytes=8 << 20),
        name="scale_levels",
    )(grid, packed, stats)


def solution(mesh):
    sizes = tuple(mesh.shape[a] for a in AXES)
    spec = P(*AXES)
    return jax.shard_map(
        functools.partial(per_device, sizes),
        mesh=mesh,
        in_specs=(spec,),
        out_specs=(spec,) * 5 + (P(),),
        check_vma=False,
    )
```

```python
import functools

import jax
import jax.numpy as jnp
import numpy as np
from jax import lax
from jax.experimental import pallas as pl
from jax.experimental.pallas import tpu as pltpu
from jax.sharding import PartitionSpec as P

LEVELS = 5
EPSILON = 1e-06
LANES = 128
PAD = 8
CHUNKS = 4
AXES = ("gx", "gy", "gz")
MESH = pl.DeviceIdType.MESH
HOPS = ((1, 1, 1), (1, 0, 1), (0, 1, 1), (0, 0, 1), (1, 0, 0), (1, 1, 0), (0, 1, 0))


def round_up(n, m):
    return -(-n // m) * m


class Plan:
    def __init__(self, shape):
        self.nx, self.ny, self.nz = shape
        self.xs = [self.nx >> l for l in range(1, LEVELS + 1)]
        self.ys = [self.ny >> l for l in range(1, LEVELS + 1)]
        self.zs = [self.nz >> l for l in range(1, LEVELS + 1)]
        assert self.zs[0] == LANES and self.ys[0] % 8 == 0
        self.ext = [round_up(y + 1, 8) for y in self.ys]
        self.pys = [round_up(y, 8) for y in self.ys]
        self.coff = [0] + np.concatenate([[0], np.cumsum(self.zs[1:])]).tolist()
        self.end = self.coff[-1]
        self.tail = [self.end + LEVELS - 1] + [self.end + l for l in range(LEVELS - 1)]
        assert self.end + LEVELS <= LANES
        self.zoff = [0, 1]
        for l in range(1, LEVELS):
            self.zoff.append(self.zoff[l] + self.xs[l] * self.pys[l] // 8)
        assert self.xs[0] * self.ys[0] // 8 <= LANES and self.zoff[-1] <= self.xs[0] * 2
        firsts = [self.zoff[l] + g * self.xs[l] for l in range(1, LEVELS) for g in range(self.pys[l] // 8)]
        assert all(f % self.xs[0] for f in firsts)
        rows = [x * p for x, p in zip(self.xs[1:], self.pys[1:])]
        self.base = [0] + np.concatenate([[0], np.cumsum(rows)]).tolist()
        self.own = self.base[-1]
        self.stage = [PAD + max(self.ext[l - 1], 2 * self.ext[l]) for l in range(1, LEVELS)]

    def fill(self, table):
        col = lax.broadcasted_iota(jnp.int32, (1, 2 * LANES), 1)
        width = jnp.full((1, 2 * LANES), 2, jnp.int32)
        cell = col
        for l in range(1, LEVELS):
            inside = col >= LANES + self.coff[l]
            width = jnp.where(inside, 2 << l, width)
            cell = jnp.where(inside, col - (LANES + self.coff[l]), cell)
        for l in range(LEVELS):
            inside = col == LANES + self.tail[l]
            width = jnp.where(inside, 2 << l, width)
            cell = jnp.where(inside, self.zs[l], cell)
        inside = (col < LANES + self.end + LEVELS).astype(jnp.float32)
        at, width = (width * cell).astype(jnp.float32), width.astype(jnp.float32)
        factor = inside / (16.0 * width * width)
        step = 64
        for r in range(0, self.nz, step):
            z = lax.broadcasted_iota(jnp.int32, (step, 2 * LANES), 0) + r
            hat = jnp.maximum(width - jnp.abs(z.astype(jnp.float32) - at), 0.0)
            table[r : r + step, :] = (hat * factor).astype(jnp.bfloat16)


def halves(x):
    hi = x.astype(jnp.bfloat16)
    return hi, (x - hi.astype(jnp.float32)).astype(jnp.bfloat16)


def dot(a, b):
    return lax.dot_general(a, b, (((1,), (0,)), ((), ())), preferred_element_type=jnp.float32)


def roll(x, shift):
    shift %= LANES
    return pltpu.roll(x, shift, 1) if shift else x


def gather_kernel(plan, sizes, *refs):
    p = plan
    v_hbm = refs[0]
    out1, outc, stats = refs[1:4]
    vin, table = refs[4:6]
    stages = refs[6:10]
    sends = refs[10:17]
    recvs = refs[17:24]
    mine, parts = refs[24:26]
    vsem, ssem, rsem, asend, arecv = refs[26:31]
    f32 = jnp.float32
    pos = [lax.axis_index(a) for a in AXES]
    group = sizes[0] * sizes[1]
    me = pos[0] * sizes[1] + pos[1]
    x1, y1 = p.xs[0], p.ys[0]

    in_plane = []
    for k in range(group):
        r = lax.rem(me + k, group)
        in_plane.append((r // sizes[1], lax.rem(r, sizes[1])))
    in_line = [lax.rem(pos[2] + k, sizes[2]) for k in range(sizes[2])]
    others = [
        {"gx": gx, "gy": gy, "gz": gz} for gz in in_line for gx, gy in in_plane
    ][1:]

    def along(hop, way):
        ok, target = None, {}
        for a in range(3):
            target[AXES[a]] = pos[a]
            if hop[a]:
                here = pos[a] < sizes[a] - 1 if way > 0 else pos[a] > 0
                ok = here if ok is None else jnp.logical_and(ok, here)
                target[AXES[a]] = lax.rem(pos[a] + way + sizes[a], sizes[a])
        return ok, target

    per = p.nx // CHUNKS
    vcopies = [
        [
            pltpu.make_async_copy(
                v_hbm.at[pl.ds(c * per, per), :, pl.ds(h * LANES, LANES)],
                vin.at[pl.ds(c * per, per), h, pl.ds(PAD, p.ny)],
                vsem.at[2 * c + h],
            )
            for h in range(2)
        ]
        for c in range(CHUNKS)
    ]
    for pair in vcopies:
        for c in pair:
            c.start()

    barrier = pltpu.get_barrier_semaphore()
    for target in others:
        pl.semaphore_signal(barrier, inc=1, device_id=target, device_id_type=MESH)

    p.fill(table)
    after = PAD + p.ny
    for x in range(p.nx):
        for h in range(2):
            vin[x, h, 0:PAD, :] = jnp.zeros((PAD, LANES), f32)
            vin[x, h, after:, :] = jnp.zeros((2 * PAD, LANES), f32)
    for l in range(1, LEVELS):
        s = stages[l - 1]
        for k in range(p.xs[l] + 1):
            s[k, 0:PAD, :] = jnp.zeros((PAD, LANES), f32)
            rest = p.stage[l - 1] - PAD - p.ext[l - 1]
            if rest:
                s[k, PAD + p.ext[l - 1] :, :] = jnp.zeros((rest, LANES), f32)

    def plane_of(x):
        cols = []
        for h in range(2):
            even = vin[x, h, pl.ds(PAD, y1, 2), :]
            odd = vin[x, h, pl.ds(PAD + 1, y1, 2), :]
            prev = vin[x, h, pl.ds(PAD - 1, y1, 2), :]
            last = vin[x, h, pl.ds(after - 1, 8, 2), :]
            cols.append(jnp.concatenate([(even + even) + (odd + prev), last], axis=0))
        return jnp.concatenate(cols, axis=1)

    def lanes_of(n):
        return lax.broadcasted_iota(jnp.int32, (n, LANES), 1)

    def fold_x(planes, k, n):
        if k == n:
            return 0.25 * planes[2 * k - 1] + 0.5 * planes[2 * k]
        sides = planes[2 * k + 1] + planes[2 * k - 1] if k else planes[1]
        return 0.5 * planes[2 * k] + 0.25 * sides

    def fold_y(s, k, n):
        even = s[k, pl.ds(PAD, n, 2), :]
        odd = s[k, pl.ds(PAD + 1, n, 2), :]
        prev = s[k, pl.ds(PAD - 1, n, 2), :]
        return 0.5 * even + 0.25 * (odd + prev)

    xyz, zx, yz, zf, xf, xy, yf = sends
    half = per // 2
    rows = p.ext[0]
    comps = []
    lane = lanes_of(8)
    row = lax.broadcasted_iota(jnp.int32, (8, LANES), 0)
    blank = jnp.zeros((8, LANES), f32)
    faces = {"zf": [blank, blank], "zx": [blank, blank], "yz": [], "xyz": []}

    def collect(l, planes, first, line):
        n, block = p.xs[l], min(l, 1)
        for i, plane in enumerate(planes, first):
            z, y = ("zf", "yz") if i < n else ("zx", "xyz")
            for g in range(p.pys[l] // 8):
                to = p.zoff[l] + g * n + i % n
                moved = roll(plane[8 * g : 8 * g + 8], to - p.tail[l])
                faces[z][block] = jnp.where(lane == to, moved, faces[z][block])
            to = p.zoff[l] + i % n
            g = p.ys[l] // 8
            moved = roll(plane[8 * g : 8 * g + 8], to - p.tail[l])
            line[y] = jnp.where(lane == to, moved, line[y])

    def close(l, line):
        s = p.ys[l] % 8
        for y in ("yz", "xyz"):
            faces[y].append(line[y][s : s + 1])

    before = None
    line = {"yz": blank, "xyz": blank}
    for c in range(CHUNKS):
        for copy in vcopies[c]:
            copy.wait()
        us = []
        for j in range(half):
            i = c * half + j
            even, odd = plane_of(2 * i), plane_of(2 * i + 1)
            t = (even + even) + odd
            us.append(t if before is None else t + before)
            before = odd
        if c == CHUNKS - 1:
            us.append(before)
        count = len(us)
        if count * rows % 16:
            us.append(jnp.zeros((8, p.nz), f32))
        hi, lo = halves(jnp.concatenate(us, axis=0))
        z = dot(hi, table[...]) + dot(lo, table[...])
        for j in range(count):
            i = c * half + j
            plane = z[j * rows : (j + 1) * rows]
            comp = plane[:, LANES:]
            comps.append(comp)
            collect(0, [comp], i, line)
            if i < x1:
                out1[i] = plane[:y1, :LANES]
                yf[i : i + 1, :] = plane[y1 : y1 + 1, :LANES]
            else:
                xf[0:y1, :] = plane[:y1, :LANES]
                xy[0:1, :] = plane[y1 : y1 + 1, :LANES]
            if i % 2 or i == x1:
                stages[0][i // 2, PAD : PAD + rows, :] = fold_x(comps, i // 2, p.xs[1])

    close(0, line)
    grids = [None]
    for l in range(1, LEVELS):
        n, e = p.xs[l], p.ext[l]
        planes = [fold_y(stages[l - 1], k, e) for k in range(n + 1)]
        line = {"yz": blank, "xyz": blank}
        collect(l, planes, 0, line)
        close(l, line)
        grids.append(planes)
        if l + 1 < LEVELS:
            for k in range(p.xs[l + 1] + 1):
                stages[l][k, PAD : PAD + e, :] = fold_x(planes, k, p.xs[l + 1])

    def pick(pieces):
        n = pieces[0][1].shape[0]
        lane = lanes_of(n)
        out = pieces[0][1]
        for l, x in pieces[1:]:
            out = jnp.where(lane >= p.coff[l], x, out)
        return out

    zf[0:8, :] = faces["zf"][0]
    zf[8:16, :] = faces["zf"][1]
    zx[...] = faces["zx"][0] + faces["zx"][1]
    for name, ref in (("yz", yz), ("xyz", xyz)):
        ref[0:1, :] = faces[name][0]
        ref[1:2, :] = functools.reduce(jnp.add, faces[name][1:])
    levels = range(1, LEVELS)
    for g in range(p.pys[1] // 8):
        at = y1 + 8 * g
        xf[at : at + 8, :] = pick(
            [
                (l, grids[l][p.xs[l]][8 * g : 8 * g + 8])
                for l in levels
                if 8 * g + 8 <= p.pys[l]
            ]
        )
    xy[1:2, :] = pick([(l, grids[l][p.xs[l]][p.ys[l] : p.ys[l] + 1]) for l in levels])
    for k in range(p.xs[1]):
        yf[x1 + k : x1 + k + 1, :] = pick(
            [(l, grids[l][k][p.ys[l] : p.ys[l] + 1]) for l in levels if k < p.xs[l]]
        )
    for l in levels:
        q = p.pys[l]
        for k in range(p.xs[l]):
            outc[p.base[l] + k * q : p.base[l] + (k + 1) * q, :] = grids[l][k][:q]

    pl.semaphore_wait(barrier, len(others))

    has_next, has_prev, copies = [], [], []
    for n, hop in enumerate(HOPS):
        ok_n, target = along(hop, 1)
        has_next.append(ok_n)
        has_prev.append(along(hop, -1)[0])
        copies.append(
            pltpu.make_async_remote_copy(
                src_ref=sends[n],
                dst_ref=recvs[n],
                send_sem=ssem.at[n],
                recv_sem=rsem.at[n],
                device_id=target,
                device_id_type=MESH,
            )
        )
    for n in range(len(HOPS)):

        @pl.when(has_next[n])
        def _():
            copies[n].start()

    for n in range(len(HOPS)):

        @pl.when(jnp.logical_not(has_prev[n]))
        def _():
            recvs[n][...] = jnp.zeros(recvs[n].shape, f32)

    for n in range(len(HOPS)):

        @pl.when(has_prev[n])
        def _():
            copies[n].wait_recv()

    rxyz, rzx, ryz, rzf, rxf, rxy, ryf = recvs
    top = row == 0
    mine_first = lane % x1 == 0
    lines = ryz[...] + rxyz[...]
    col1 = rzf[0:8, :] + jnp.where(mine_first, rzx[...], 0.0) + jnp.where(top, lines[0:1], 0.0)
    col2 = rzf[8:16, :] + jnp.where(mine_first, 0.0, rzx[...]) + jnp.where(top, lines[1:2], 0.0)
    acc = jnp.zeros((8, LANES), f32)
    for i in range(x1):
        edge = ryf[i : i + 1, :]
        if i == 0:
            edge = edge + rxy[0:1, :]
        for g in range(y1 // 8):
            part = out1[i, 8 * g : 8 * g + 8, :]
            if i == 0:
                part = part + rxf[8 * g : 8 * g + 8, :]
            if g == 0:
                part = part + jnp.where(top, edge, 0.0)
            part = part + jnp.where(lane == 0, roll(col1, -(g * x1 + i)), 0.0)
            out1[i, 8 * g : 8 * g + 8, :] = part
            acc = acc + part * part
    mine[0:1, :] = jnp.sum(acc, axis=0, keepdims=True)
    acc = jnp.zeros((8, LANES), f32)
    for l in levels:
        q = p.pys[l]
        keep = (lane >= p.coff[l]) & (lane < p.coff[l + 1] if l + 1 < LEVELS else lane < p.end)
        if p.ys[l] < 8:
            keep = keep & (row < p.ys[l])
        total = jnp.zeros((8, LANES), f32)
        for k in range(p.xs[l]):
            edge = ryf[x1 + k : x1 + k + 1, :]
            if k == 0:
                edge = edge + rxy[1:2, :]
            for g in range(q // 8):
                at = p.base[l] + k * q + 8 * g
                part = outc[at : at + 8, :]
                if k == 0:
                    part = part + rxf[y1 + 8 * g : y1 + 8 * g + 8, :]
                if g == 0:
                    part = part + jnp.where(top, edge, 0.0)
                shifted = roll(col2, p.coff[l] - p.zoff[l] - g * p.xs[l] - k)
                part = part + jnp.where(lane == p.coff[l], shifted, 0.0)
                outc[at : at + 8, :] = part
                total = total + part * part
        acc = jnp.where(keep, total, acc)
    mine[1:2, :] = jnp.sum(acc, axis=0, keepdims=True)

    pending = [
        pltpu.make_async_remote_copy(
            src_ref=mine,
            dst_ref=parts.at[k + 1],
            send_sem=asend.at[0],
            recv_sem=arecv.at[0],
            device_id=target,
            device_id_type=MESH,
        )
        for k, target in enumerate(others)
    ]
    for c in reversed(pending):
        c.start()
    parts[0] = mine[...]
    every = pltpu.make_async_remote_copy(
        src_ref=parts.at[pl.ds(1, len(others))],
        dst_ref=parts.at[pl.ds(1, len(others))],
        send_sem=asend.at[0],
        recv_sem=arecv.at[0],
        device_id=others[0],
        device_id_type=MESH,
    )
    every.wait_recv()
    stats[...] = jnp.sum(parts[...], axis=0)
    every.wait_send()
    for n in range(len(HOPS)):

        @pl.when(has_next[n])
        def _():
            copies[n].wait_send()


def scale_kernel(plan, devices, grid, packed, stats, o1, o2, o3, o4, o5, scales):
    p = plan
    lane1 = lax.broadcasted_iota(jnp.int32, (1, LANES), 1)
    outs = (o1, o2, o3, o4, o5)
    square = jnp.ones((1, 1), jnp.float32)
    for l in range(LEVELS):
        row = stats[0:1, :] if l == 0 else stats[1:2, :]
        if l:
            end = p.coff[l] + p.zs[l]
            row = jnp.where((lane1 >= p.coff[l]) & (lane1 < end), row, 0.0)
        cells = devices * p.xs[l] * p.ys[l] * p.zs[l]
        mean = jnp.sum(row, axis=1, keepdims=True) * (1.0 / cells)
        before, square = square, mean + EPSILON * square
        scales[l] = jnp.sqrt(square / before)[0, 0]
        inverse = 1.0 / jnp.sqrt(square)
        if l == 0:
            o1[...] = grid[...] * inverse.reshape(1, 1, 1)
            continue
        block = packed[p.base[l] : p.base[l + 1], :] * inverse
        block = roll(block, -p.coff[l])
        block = block.reshape(p.xs[l], p.pys[l], LANES)
        outs[l][...] = block[:, : p.ys[l], : p.zs[l]]


def per_device(sizes, residual_in):
    plan = Plan(residual_in.shape)
    p = plan
    count = sizes[0] * sizes[1] * sizes[2]
    f32, bf16 = jnp.float32, jnp.bfloat16
    long = p.ys[0] + p.pys[1]
    messages = [(2, LANES), (8, LANES), (2, LANES), (16, LANES)]
    messages += [(long, LANES), (2, LANES), (p.xs[0] + p.xs[1], LANES)]
    anywhere = pl.BlockSpec(memory_space=pl.ANY)
    vmem = pl.BlockSpec(memory_space=pltpu.VMEM)
    dma = pltpu.SemaphoreType.DMA
    grid, packed, stats = pl.pallas_call(
        functools.partial(gather_kernel, p, sizes),
        out_shape=(
            jax.ShapeDtypeStruct((p.xs[0], p.ys[0], p.zs[0]), f32),
            jax.ShapeDtypeStruct((p.own, LANES), f32),
            jax.ShapeDtypeStruct((2, LANES), f32),
        ),
        in_specs=[anywhere],
        out_specs=(vmem, vmem, vmem),
        scratch_shapes=[
            pltpu.VMEM((p.nx, 2, p.ny + 3 * PAD, LANES), f32),
            pltpu.VMEM((p.nz, 2 * LANES), bf16),
        ]
        + [pltpu.VMEM((p.xs[l] + 1, p.stage[l - 1], LANES), f32) for l in range(1, LEVELS)]
        + [pltpu.VMEM(s, f32) for s in messages]
        + [pltpu.VMEM(s, f32) for s in messages]
        + [
            pltpu.VMEM((2, LANES), f32),
            pltpu.VMEM((count, 2, LANES), f32),
            dma((2 * CHUNKS,)),
            dma((len(HOPS),)),
            dma((len(HOPS),)),
            dma((1,)),
            dma((1,)),
        ],
        compiler_params=pltpu.CompilerParams(
            collective_id=0, has_side_effects=True, vmem_limit_bytes=51 << 20
        ),
        name="restrict_exchange",
    )(residual_in)
    shapes = list(zip(p.xs, p.ys, p.zs))
    return pl.pallas_call(
        functools.partial(scale_kernel, p, count),
        out_shape=tuple(jax.ShapeDtypeStruct(s, f32) for s in shapes)
        + (jax.ShapeDtypeStruct((LEVELS,), f32),),
        in_specs=[vmem] * 3,
        out_specs=(vmem,) * 5 + (pl.BlockSpec(memory_space=pltpu.SMEM),),
        compiler_params=pltpu.CompilerParams(vmem_limit_bytes=8 << 20),
        name="scale_levels",
    )(grid, packed, stats)


def solution(mesh):
    sizes = tuple(mesh.shape[a] for a in AXES)
    spec = P(*AXES)
    return jax.shard_map(
        functools.partial(per_device, sizes),
        mesh=mesh,
        in_specs=(spec,),
        out_specs=(spec,) * 5 + (P(),),
        check_vma=False,
    )
```

```python
import functools

import jax
import jax.numpy as jnp
import numpy as np
from jax import lax
from jax.experimental import pallas as pl
from jax.experimental.pallas import tpu as pltpu
from jax.sharding import PartitionSpec as P

LEVELS = 5
EPSILON = 1e-06
LANES = 128
PAD = 8
CHUNKS = (1, 1)
AXES = ("gx", "gy", "gz")
MESH = pl.DeviceIdType.MESH
HOPS = ((1, 1, 1), (1, 0, 1), (0, 1, 1), (0, 0, 1), (1, 0, 0), (1, 1, 0), (0, 1, 0))


def round_up(n, m):
    return -(-n // m) * m


class Plan:
    def __init__(self, shape):
        self.nx, self.ny, self.nz = shape
        self.xs = [self.nx >> l for l in range(1, LEVELS + 1)]
        self.ys = [self.ny >> l for l in range(1, LEVELS + 1)]
        self.zs = [self.nz >> l for l in range(1, LEVELS + 1)]
        assert self.zs[0] == LANES and self.ys[0] % 8 == 0
        self.ext = [round_up(y + 1, 8) for y in self.ys]
        self.pys = [round_up(y, 8) for y in self.ys]
        self.coff = [0] + np.concatenate([[0], np.cumsum(self.zs[1:])]).tolist()
        self.end = self.coff[-1]
        self.tail = [self.end + LEVELS - 1] + [self.end + l for l in range(LEVELS - 1)]
        assert self.end + LEVELS <= LANES
        self.zoff = [0, 1]
        for l in range(1, LEVELS):
            self.zoff.append(self.zoff[l] + self.xs[l] * self.pys[l] // 8)
        assert self.xs[0] * self.ys[0] // 8 <= LANES and self.zoff[-1] <= self.xs[0] * 2
        firsts = [self.zoff[l] + g * self.xs[l] for l in range(1, LEVELS) for g in range(self.pys[l] // 8)]
        assert all(f % self.xs[0] for f in firsts)
        rows = [x * p for x, p in zip(self.xs[1:], self.pys[1:])]
        self.base = [0] + np.concatenate([[0], np.cumsum(rows)]).tolist()
        self.own = self.base[-1]
        self.stage = [PAD + max(self.ext[l - 1], 2 * self.ext[l]) for l in range(1, LEVELS)]

    def fill(self, table):
        col = lax.broadcasted_iota(jnp.int32, (1, 2 * LANES), 1)
        width = jnp.full((1, 2 * LANES), 2, jnp.int32)
        cell = col
        for l in range(1, LEVELS):
            inside = col >= LANES + self.coff[l]
            width = jnp.where(inside, 2 << l, width)
            cell = jnp.where(inside, col - (LANES + self.coff[l]), cell)
        for l in range(LEVELS):
            inside = col == LANES + self.tail[l]
            width = jnp.where(inside, 2 << l, width)
            cell = jnp.where(inside, self.zs[l], cell)
        inside = (col < LANES + self.end + LEVELS).astype(jnp.float32)
        at, width = (width * cell).astype(jnp.float32), width.astype(jnp.float32)
        factor = inside / (16.0 * width * width)
        step = 64
        for r in range(0, self.nz, step):
            z = lax.broadcasted_iota(jnp.int32, (step, 2 * LANES), 0) + r
            hat = jnp.maximum(width - jnp.abs(z.astype(jnp.float32) - at), 0.0)
            table[r : r + step, :] = (hat * factor).astype(jnp.bfloat16)


def halves(x):
    hi = x.astype(jnp.bfloat16)
    return hi, (x - hi.astype(jnp.float32)).astype(jnp.bfloat16)


def dot(a, b):
    return lax.dot_general(a, b, (((1,), (0,)), ((), ())), preferred_element_type=jnp.float32)


def roll(x, shift):
    shift %= LANES
    return pltpu.roll(x, shift, 1) if shift else x


def gather_kernel(plan, sizes, *refs):
    p = plan
    v_hbm = refs[0]
    out1, outc, stats = refs[1:4]
    vin, table = refs[4:6]
    stages = refs[6:10]
    sends = refs[10:17]
    recvs = refs[17:24]
    mine, parts = refs[24:26]
    vsem, ssem, rsem, asend, arecv = refs[26:31]
    f32 = jnp.float32
    pos = [lax.axis_index(a) for a in AXES]
    group = sizes[0] * sizes[1]
    me = pos[0] * sizes[1] + pos[1]
    x1, y1 = p.xs[0], p.ys[0]

    in_plane = []
    for k in range(group):
        r = lax.rem(me + k, group)
        in_plane.append((r // sizes[1], lax.rem(r, sizes[1])))
    others, slots = [], []
    for k in range(sizes[2]):
        rest = sizes[2] - 1 - k
        gz = pos[2]
        if rest:
            low = k + (k >= pos[2]).astype(jnp.int32)
            high = rest - (rest <= pos[2]).astype(jnp.int32)
            gz = jnp.where(2 * pos[2] >= sizes[2], low, high)
        slot = lax.rem(gz - pos[2] + sizes[2], sizes[2]) * group
        for n in reversed(range(0 if rest else 1, group)):
            gx, gy = in_plane[n]
            others.append({"gx": gx, "gy": gy, "gz": gz})
            slots.append(slot + n)

    def along(hop, way):
        ok, target = None, {}
        for a in range(3):
            target[AXES[a]] = pos[a]
            if hop[a]:
                here = pos[a] < sizes[a] - 1 if way > 0 else pos[a] > 0
                ok = here if ok is None else jnp.logical_and(ok, here)
                target[AXES[a]] = lax.rem(pos[a] + way + sizes[a], sizes[a])
        return ok, target

    unit = p.nx // sum(CHUNKS)
    starts = [unit * sum(CHUNKS[:c]) for c in range(len(CHUNKS) + 1)]
    spans = [pl.ds(a, b - a) for a, b in zip(starts, starts[1:])]
    vcopies = [
        [
            pltpu.make_async_copy(
                v_hbm.at[span, :, pl.ds(h * LANES, LANES)],
                vin.at[span, h, pl.ds(PAD, p.ny)],
                vsem.at[2 * c + h],
            )
            for h in range(2)
        ]
        for c, span in enumerate(spans)
    ]
    for pair in vcopies:
        for c in pair:
            c.start()

    barrier = pltpu.get_barrier_semaphore()
    for target in others:
        pl.semaphore_signal(barrier, inc=1, device_id=target, device_id_type=MESH)

    p.fill(table)
    after = PAD + p.ny
    for x in range(p.nx):
        for h in range(2):
            vin[x, h, 0:PAD, :] = jnp.zeros((PAD, LANES), f32)
            vin[x, h, after:, :] = jnp.zeros((2 * PAD, LANES), f32)
    for l in range(1, LEVELS):
        s = stages[l - 1]
        for k in range(p.xs[l] + 1):
            s[k, 0:PAD, :] = jnp.zeros((PAD, LANES), f32)
            rest = p.stage[l - 1] - PAD - p.ext[l - 1]
            if rest:
                s[k, PAD + p.ext[l - 1] :, :] = jnp.zeros((rest, LANES), f32)

    def plane_of(x):
        cols = []
        for h in range(2):
            even = vin[x, h, pl.ds(PAD, y1, 2), :]
            odd = vin[x, h, pl.ds(PAD + 1, y1, 2), :]
            prev = vin[x, h, pl.ds(PAD - 1, y1, 2), :]
            last = vin[x, h, pl.ds(after - 1, 8, 2), :]
            cols.append(jnp.concatenate([(even + even) + (odd + prev), last], axis=0))
        return jnp.concatenate(cols, axis=1)

    def lanes_of(n):
        return lax.broadcasted_iota(jnp.int32, (n, LANES), 1)

    def fold_x(planes, k, n):
        if k == n:
            return 0.25 * planes[2 * k - 1] + 0.5 * planes[2 * k]
        sides = planes[2 * k + 1] + planes[2 * k - 1] if k else planes[1]
        return 0.5 * planes[2 * k] + 0.25 * sides

    def fold_y(s, k, n):
        even = s[k, pl.ds(PAD, n, 2), :]
        odd = s[k, pl.ds(PAD + 1, n, 2), :]
        prev = s[k, pl.ds(PAD - 1, n, 2), :]
        return 0.5 * even + 0.25 * (odd + prev)

    xyz, zx, yz, zf, xf, xy, yf = sends
    rows = p.ext[0]
    comps = []
    lane = lanes_of(8)
    row = lax.broadcasted_iota(jnp.int32, (8, LANES), 0)
    blank = jnp.zeros((8, LANES), f32)
    faces = {"zf": [blank, blank], "zx": [blank, blank], "yz": [], "xyz": []}

    def collect(l, planes, first, line):
        n, block = p.xs[l], min(l, 1)
        for i, plane in enumerate(planes, first):
            z, y = ("zf", "yz") if i < n else ("zx", "xyz")
            for g in range(p.pys[l] // 8):
                to = p.zoff[l] + g * n + i % n
                moved = roll(plane[8 * g : 8 * g + 8], to - p.tail[l])
                faces[z][block] = jnp.where(lane == to, moved, faces[z][block])
            to = p.zoff[l] + i % n
            g = p.ys[l] // 8
            moved = roll(plane[8 * g : 8 * g + 8], to - p.tail[l])
            line[y] = jnp.where(lane == to, moved, line[y])

    def close(l, line):
        s = p.ys[l] % 8
        for y in ("yz", "xyz"):
            faces[y].append(line[y][s : s + 1])

    before = None
    line = {"yz": blank, "xyz": blank}
    for c in range(len(CHUNKS)):
        first, half = starts[c] // 2, (starts[c + 1] - starts[c]) // 2
        for copy in vcopies[c]:
            copy.wait()
        us = []
        for j in range(half):
            i = first + j
            even, odd = plane_of(2 * i), plane_of(2 * i + 1)
            t = (even + even) + odd
            us.append(t if before is None else t + before)
            before = odd
        if c == len(CHUNKS) - 1:
            us.append(before)
        count = len(us)
        if count * rows % 16:
            us.append(jnp.zeros((8, p.nz), f32))
        hi, lo = halves(jnp.concatenate(us, axis=0))
        z = dot(hi, table[...]) + dot(lo, table[...])
        for j in range(count):
            i = first + j
            plane = z[j * rows : (j + 1) * rows]
            comp = plane[:, LANES:]
            comps.append(comp)
            collect(0, [comp], i, line)
            if i < x1:
                out1[i] = plane[:y1, :LANES]
                yf[i : i + 1, :] = plane[y1 : y1 + 1, :LANES]
            else:
                xf[0:y1, :] = plane[:y1, :LANES]
                xy[0:1, :] = plane[y1 : y1 + 1, :LANES]
            if i % 2 or i == x1:
                stages[0][i // 2, PAD : PAD + rows, :] = fold_x(comps, i // 2, p.xs[1])

    close(0, line)
    grids = [None]
    for l in range(1, LEVELS):
        n, e = p.xs[l], p.ext[l]
        planes = [fold_y(stages[l - 1], k, e) for k in range(n + 1)]
        line = {"yz": blank, "xyz": blank}
        collect(l, planes, 0, line)
        close(l, line)
        grids.append(planes)
        if l + 1 < LEVELS:
            for k in range(p.xs[l + 1] + 1):
                stages[l][k, PAD : PAD + e, :] = fold_x(planes, k, p.xs[l + 1])

    def pick(pieces):
        n = pieces[0][1].shape[0]
        lane = lanes_of(n)
        out = pieces[0][1]
        for l, x in pieces[1:]:
            out = jnp.where(lane >= p.coff[l], x, out)
        return out

    zf[0:8, :] = faces["zf"][0]
    zf[8:16, :] = faces["zf"][1]
    zx[...] = faces["zx"][0] + faces["zx"][1]
    for name, ref in (("yz", yz), ("xyz", xyz)):
        ref[0:1, :] = faces[name][0]
        ref[1:2, :] = functools.reduce(jnp.add, faces[name][1:])
    levels = range(1, LEVELS)
    for g in range(p.pys[1] // 8):
        at = y1 + 8 * g
        xf[at : at + 8, :] = pick(
            [
                (l, grids[l][p.xs[l]][8 * g : 8 * g + 8])
                for l in levels
                if 8 * g + 8 <= p.pys[l]
            ]
        )
    xy[1:2, :] = pick([(l, grids[l][p.xs[l]][p.ys[l] : p.ys[l] + 1]) for l in levels])
    for k in range(p.xs[1]):
        yf[x1 + k : x1 + k + 1, :] = pick(
            [(l, grids[l][k][p.ys[l] : p.ys[l] + 1]) for l in levels if k < p.xs[l]]
        )
    for l in levels:
        q = p.pys[l]
        for k in range(p.xs[l]):
            outc[p.base[l] + k * q : p.base[l] + (k + 1) * q, :] = grids[l][k][:q]

    pl.semaphore_wait(barrier, len(others))

    has_next, has_prev, copies = [], [], []
    for n, hop in enumerate(HOPS):
        ok_n, target = along(hop, 1)
        has_next.append(ok_n)
        has_prev.append(along(hop, -1)[0])
        copies.append(
            pltpu.make_async_remote_copy(
                src_ref=sends[n],
                dst_ref=recvs[n],
                send_sem=ssem.at[n],
                recv_sem=rsem.at[n],
                device_id=target,
                device_id_type=MESH,
            )
        )
    for n in range(len(HOPS)):

        @pl.when(has_next[n])
        def _():
            copies[n].start()

    for n in range(len(HOPS)):

        @pl.when(jnp.logical_not(has_prev[n]))
        def _():
            recvs[n][...] = jnp.zeros(recvs[n].shape, f32)

    for n in range(len(HOPS)):

        @pl.when(has_prev[n])
        def _():
            copies[n].wait_recv()

    rxyz, rzx, ryz, rzf, rxf, rxy, ryf = recvs
    top = row == 0
    mine_first = lane % x1 == 0
    lines = ryz[...] + rxyz[...]
    col1 = rzf[0:8, :] + jnp.where(mine_first, rzx[...], 0.0) + jnp.where(top, lines[0:1], 0.0)
    col2 = rzf[8:16, :] + jnp.where(mine_first, 0.0, rzx[...]) + jnp.where(top, lines[1:2], 0.0)
    acc = jnp.zeros((8, LANES), f32)
    for i in range(x1):
        edge = ryf[i : i + 1, :]
        if i == 0:
            edge = edge + rxy[0:1, :]
        for g in range(y1 // 8):
            part = out1[i, 8 * g : 8 * g + 8, :]
            if i == 0:
                part = part + rxf[8 * g : 8 * g + 8, :]
            if g == 0:
                part = part + jnp.where(top, edge, 0.0)
            part = part + jnp.where(lane == 0, roll(col1, -(g * x1 + i)), 0.0)
            out1[i, 8 * g : 8 * g + 8, :] = part
            acc = acc + part * part
    mine[0:1, :] = jnp.sum(acc, axis=0, keepdims=True)
    acc = jnp.zeros((8, LANES), f32)
    for l in levels:
        q = p.pys[l]
        keep = (lane >= p.coff[l]) & (lane < p.coff[l + 1] if l + 1 < LEVELS else lane < p.end)
        if p.ys[l] < 8:
            keep = keep & (row < p.ys[l])
        total = jnp.zeros((8, LANES), f32)
        for k in range(p.xs[l]):
            edge = ryf[x1 + k : x1 + k + 1, :]
            if k == 0:
                edge = edge + rxy[1:2, :]
            for g in range(q // 8):
                at = p.base[l] + k * q + 8 * g
                part = outc[at : at + 8, :]
                if k == 0:
                    part = part + rxf[y1 + 8 * g : y1 + 8 * g + 8, :]
                if g == 0:
                    part = part + jnp.where(top, edge, 0.0)
                shifted = roll(col2, p.coff[l] - p.zoff[l] - g * p.xs[l] - k)
                part = part + jnp.where(lane == p.coff[l], shifted, 0.0)
                outc[at : at + 8, :] = part
                total = total + part * part
        acc = jnp.where(keep, total, acc)
    mine[1:2, :] = jnp.sum(acc, axis=0, keepdims=True)

    pending = [
        pltpu.make_async_remote_copy(
            src_ref=mine,
            dst_ref=parts.at[slot],
            send_sem=asend.at[0],
            recv_sem=arecv.at[0],
            device_id=target,
            device_id_type=MESH,
        )
        for target, slot in zip(others, slots)
    ]
    for c in pending:
        c.start()
    parts[0] = mine[...]
    every = pltpu.make_async_remote_copy(
        src_ref=parts.at[pl.ds(1, len(others))],
        dst_ref=parts.at[pl.ds(1, len(others))],
        send_sem=asend.at[0],
        recv_sem=arecv.at[0],
        device_id=others[0],
        device_id_type=MESH,
    )
    every.wait_recv()
    stats[...] = jnp.sum(parts[...], axis=0)
    every.wait_send()
    for n in range(len(HOPS)):

        @pl.when(has_next[n])
        def _():
            copies[n].wait_send()


def scale_kernel(plan, devices, grid, packed, stats, o1, o2, o3, o4, o5, scales):
    p = plan
    lane1 = lax.broadcasted_iota(jnp.int32, (1, LANES), 1)
    outs = (o1, o2, o3, o4, o5)
    square = jnp.ones((1, 1), jnp.float32)
    found = jnp.zeros((1, LANES), jnp.float32)
    for l in range(LEVELS):
        row = stats[0:1, :] if l == 0 else stats[1:2, :]
        if l:
            end = p.coff[l] + p.zs[l]
            row = jnp.where((lane1 >= p.coff[l]) & (lane1 < end), row, 0.0)
        cells = devices * p.xs[l] * p.ys[l] * p.zs[l]
        mean = jnp.sum(row, axis=1, keepdims=True) * (1.0 / cells)
        before, square = square, mean + EPSILON * square
        found = jnp.where(lane1 == l, jnp.sqrt(square / before), found)
        inverse = 1.0 / jnp.sqrt(square)
        if l == 0:
            o1[...] = grid[...] * inverse.reshape(1, 1, 1)
            continue
        block = packed[p.base[l] : p.base[l + 1], :] * inverse
        block = roll(block, -p.coff[l])
        block = block.reshape(p.xs[l], p.pys[l], LANES)
        outs[l][...] = block[:, : p.ys[l], : p.zs[l]]
    scales[...] = found[:, :LEVELS]


def per_device(sizes, residual_in):
    plan = Plan(residual_in.shape)
    p = plan
    count = sizes[0] * sizes[1] * sizes[2]
    f32, bf16 = jnp.float32, jnp.bfloat16
    long = p.ys[0] + p.pys[1]
    messages = [(2, LANES), (8, LANES), (2, LANES), (16, LANES)]
    messages += [(long, LANES), (2, LANES), (p.xs[0] + p.xs[1], LANES)]
    anywhere = pl.BlockSpec(memory_space=pl.ANY)
    vmem = pl.BlockSpec(memory_space=pltpu.VMEM)
    dma = pltpu.SemaphoreType.DMA
    grid, packed, stats = pl.pallas_call(
        functools.partial(gather_kernel, p, sizes),
        out_shape=(
            jax.ShapeDtypeStruct((p.xs[0], p.ys[0], p.zs[0]), f32),
            jax.ShapeDtypeStruct((p.own, LANES), f32),
            jax.ShapeDtypeStruct((2, LANES), f32),
        ),
        in_specs=[anywhere],
        out_specs=(vmem, vmem, vmem),
        scratch_shapes=[
            pltpu.VMEM((p.nx, 2, p.ny + 3 * PAD, LANES), f32),
            pltpu.VMEM((p.nz, 2 * LANES), bf16),
        ]
        + [pltpu.VMEM((p.xs[l] + 1, p.stage[l - 1], LANES), f32) for l in range(1, LEVELS)]
        + [pltpu.VMEM(s, f32) for s in messages]
        + [pltpu.VMEM(s, f32) for s in messages]
        + [
            pltpu.VMEM((2, LANES), f32),
            pltpu.VMEM((count, 2, LANES), f32),
            dma((2 * len(CHUNKS),)),
            dma((len(HOPS),)),
            dma((len(HOPS),)),
            dma((1,)),
            dma((1,)),
        ],
        compiler_params=pltpu.CompilerParams(
            collective_id=0, has_side_effects=True, vmem_limit_bytes=51 << 20
        ),
        name="restrict_exchange",
    )(residual_in)
    shapes = list(zip(p.xs, p.ys, p.zs))
    *grids, scales = pl.pallas_call(
        functools.partial(scale_kernel, p, count),
        out_shape=tuple(jax.ShapeDtypeStruct(s, f32) for s in shapes)
        + (jax.ShapeDtypeStruct((1, LEVELS), f32),),
        in_specs=[vmem] * 3,
        out_specs=(vmem,) * 6,
        compiler_params=pltpu.CompilerParams(vmem_limit_bytes=8 << 20),
        name="scale_levels",
    )(grid, packed, stats)
    return (*grids, scales.reshape(LEVELS))


def solution(mesh):
    sizes = tuple(mesh.shape[a] for a in AXES)
    spec = P(*AXES)
    return jax.shard_map(
        functools.partial(per_device, sizes),
        mesh=mesh,
        in_specs=(spec,),
        out_specs=(spec,) * 5 + (P(),),
        check_vma=False,
    )
```
